32 devices in a mesh: seq: 8 (over z, y), head: 4 (over x, core).
Axes of the slice: x: 2, y: 2, z: 4, core: 2. Of those that a mesh axis runs over, the one named last changes fastest.
Arguments:
- head_inputs: bfloat16 [8192, 5120], P('seq', 'head'), may hold values from -6 to 6
- gate_inputs: bfloat16 [8192, 5120], P('seq', 'head'), may hold values from -6 to 6
- step_raw: bfloat16 [8192, 80], P('seq', 'head'), may hold values from -9 to 256
- decay_log: float32 [80], replicated, may hold values from -12 to 0
- state_write: bfloat16 [8192, 128], P(('seq', 'head')), may hold values from -6 to 6
- state_read: bfloat16 [8192, 128], P(('seq', 'head')), may hold values from -0.5 to 0.5
- skip_gain: float32 [80], replicated, may hold values from 0.5 to 2
- norm_gain: float32 [5120], replicated, may hold values from 0.1 to 1.9
Outputs:
- scan_output: bfloat16 [8192, 5120], P('seq', 'head')
The draws below stay inside these ranges and needn't reach their ends.
All inputs are finite; a program needn't handle non-finite values.
Results may differ from the reference program's by a relative error of at most 0.005.
Values may be sent and summed in bfloat16 or wider, within the bound.
A program may use at most 128 MiB of HBM per device.

```python
import math
import jax
import jax.numpy as jnp
from jax import lax

HEADS = 80
HEAD_DIM = 64
STATE = 128
SPAN = 256
SEQ = 8192
INNER = 5120


def decay_plan(key):
    base = jax.random.fold_in(key, 4101)
    order = jax.random.permutation(jax.random.fold_in(base, 1), HEADS)
    count = HEADS // 2
    gradual_decay = order < count
    slow_step = jnp.exp(jax.random.uniform(jax.random.fold_in(base, 2), (HEADS,), jnp.float32, jnp.log(0.1 / SEQ), jnp.log(1.0 / SEQ)))
    fast_step = jnp.exp(jax.random.uniform(jax.random.fold_in(base, 3), (HEADS,), jnp.float32, jnp.log(0.02), jnp.log(0.06)))
    per_step = jnp.where(gradual_decay, slow_step, fast_step)
    level = jnp.where(gradual_decay, -5.5, 0.0)
    decay_rate = per_step / jax.nn.softplus(level)
    noise = 0.7 * jax.random.truncated_normal(jax.random.fold_in(base, 4), -3.0, 3.0, (SEQ, HEADS), jnp.float32)
    unscaled_step_sizes = level[None, :] + noise
    chosen_locations = jax.random.randint(jax.random.fold_in(base, 5), (8,), 0, SEQ)
    token_places = jnp.arange(SEQ, dtype=jnp.int32)
    sudden_jump = jnp.any(token_places[:, None] == chosen_locations[None, :], axis=1)
    losses = jax.random.uniform(jax.random.fold_in(base, 6), (SEQ, HEADS), jnp.float32, 0.22, 0.7)
    expected_output = losses / decay_rate[None, :]
    sudden_jump_unscaled = expected_output + jnp.log(-jnp.expm1(-expected_output))
    selected_entries = sudden_jump[:, None] & gradual_decay[None, :]
    unscaled_step_sizes = jnp.where(selected_entries, sudden_jump_unscaled, unscaled_step_sizes)
    scaling = jnp.where(selected_entries, 1.0 / expected_output, 1.0)
    return (unscaled_step_sizes, jnp.log(decay_rate), scaling)


def draw_step_raw(key, part):
    unscaled_step_sizes, decay_logs, scaling = decay_plan(key)
    return unscaled_step_sizes.astype(jnp.bfloat16)


def draw_decay_log(key, part):
    unscaled_step_sizes, decay_logs, scaling = decay_plan(key)
    return decay_logs.astype(jnp.float32)


def draw_head_inputs(key, part):
    unscaled_step_sizes, decay_logs, scaling = decay_plan(key)
    noise = jax.random.truncated_normal(jax.random.fold_in(key, 77), -6.0, 6.0, (SEQ, HEADS, HEAD_DIM), jnp.float32)
    return (noise * scaling[:, :, None]).reshape(SEQ, HEADS * HEAD_DIM).astype(jnp.bfloat16)


def levels(own_key, shape, pieces, low, largest):
    loudness = 1.0
    for axis_at, shards_of in pieces:
        draws = jax.random.uniform(jax.random.fold_in(jax.random.fold_in(own_key, 6), axis_at), (shards_of,), jnp.float32, low / len(pieces), largest / len(pieces))
        loudness = loudness * jnp.repeat(jnp.exp(draws), shape[axis_at] // shards_of).reshape((-1,) + (1,) * (len(shape) - 1 - axis_at))
    return loudness


def centred(rng, extent, scale, most, pieces=(), held_as=jnp.bfloat16):
    drawn = scale * jax.random.normal(rng, extent, jnp.float32)
    if pieces:
        drawn = drawn * levels(rng, extent, pieces, -0.22, 0.18)
    return jnp.clip(drawn, -most, most).astype(held_as)


def setup_inputs(seed: int = 0) -> dict:
    key_list = jax.random.split(jax.random.key(seed), 9)
    return {
        "head_inputs": draw_head_inputs(jax.random.fold_in(key_list[8], 71), 0),
        "gate_inputs": centred(key_list[1], (SEQ, INNER), 1.0, 6.0, ((0, 8), (1, 4))),
        "step_raw": draw_step_raw(jax.random.fold_in(key_list[8], 71), 0),
        "decay_log": draw_decay_log(jax.random.fold_in(key_list[8], 71), 0),
        "state_write": centred(key_list[4], (SEQ, STATE), 1.0, 6.0, ((0, 32),)),
        "state_read": centred(key_list[5], (SEQ, STATE), STATE ** -0.5, 0.5, ((0, 32),)),
        "skip_gain": jnp.clip(jax.random.uniform(key_list[6], (HEADS,), jnp.float32, 0.5, 2.0), 0.5, 2.0),
        "norm_gain": jnp.clip(1.0 + 0.18 * jax.random.normal(key_list[7], (INNER,), jnp.float32), 0.1, 1.9),
    }


def intra_block(values, running, step_size, scores):
    length = running.shape[1]
    row_index = lax.broadcasted_iota(jnp.int32, (length, length), 0)
    col_index = lax.broadcasted_iota(jnp.int32, (length, length), 1)
    lower = col_index <= row_index
    by_head = jnp.moveaxis(running, 2, 1)
    weight_step = jnp.moveaxis(step_size, 2, 1)
    spread = by_head[:, :, :, None] - by_head[:, :, None, :]
    mixing = jnp.where(lower, jnp.exp(jnp.where(lower, spread, 0.0)), 0.0) * scores[:, None] * weight_step[:, :, None, :]
    mixing = lax.optimization_barrier(mixing.astype(jnp.bfloat16)).astype(jnp.float32)
    return jnp.einsum('khtu,kuhp->kthp', mixing, values.astype(jnp.float32))

def block_pieces(values, step_raw, writes, reads, decay_rate, skip_gain):
    tokens = values.shape[0]
    heads = decay_rate.shape[0]
    width = values.shape[1] // heads
    blocks = tokens // SPAN
    group = math.gcd(heads, 4)
    groups = heads // group
    step_size = jax.nn.softplus(step_raw.astype(jnp.float32)).reshape(blocks, SPAN, heads)
    running = jnp.cumsum(-decay_rate * step_size, axis=1)
    shaped = values.reshape(blocks, SPAN, heads, width)
    write_blocks = writes.reshape(blocks, SPAN, -1).astype(jnp.float32)
    read_blocks = reads.reshape(blocks, SPAN, -1).astype(jnp.float32)
    scores = jnp.einsum('ktn,kun->ktu', read_blocks, write_blocks)

    def per_group(item):
        return intra_block(item[0], item[1], item[2], scores)
    split_values = jnp.moveaxis(shaped.reshape(blocks, SPAN, groups, group, width), 2, 0)
    split_running = jnp.moveaxis(running.reshape(blocks, SPAN, groups, group), 2, 0)
    split_step = jnp.moveaxis(step_size.reshape(blocks, SPAN, groups, group), 2, 0)
    mixed_groups = lax.map(per_group, (split_values, split_running, split_step))
    local = jnp.moveaxis(mixed_groups, 0, 2).reshape(blocks, SPAN, heads, width)
    wide_values = shaped.astype(jnp.float32)
    local = local + skip_gain[:, None] * wide_values
    tail = jnp.exp(running[:, -1:, :] - running) * step_size
    weighted = wide_values * tail[..., None]
    weighted = lax.optimization_barrier(weighted.astype(jnp.bfloat16)).astype(jnp.float32)
    states = jnp.einsum('kuhp,kun->khpn', weighted, write_blocks, precision=lax.Precision.HIGHEST)
    return (local, running, states, running[:, -1, :], read_blocks)

def reference(head_inputs, gate_inputs, step_raw, decay_log, state_write, state_read, skip_gain, norm_gain):
    blocks = SEQ // SPAN
    decay_rate = jnp.exp(decay_log)

    def advance(carry, item):
        values, gates, raws, writes, reads = item
        local, running, states, totals, read_blocks = block_pieces(values, raws, writes, reads, decay_rate, skip_gain)
        entering = lax.optimization_barrier(carry.astype(jnp.bfloat16)).astype(jnp.float32)
        inter = jnp.einsum('ktn,hpn->kthp', read_blocks, entering, precision=lax.Precision.HIGHEST)
        ssm = (local + jnp.exp(running)[..., None] * inter).reshape(SPAN, -1)
        gated = ssm * jax.nn.silu(gates.astype(jnp.float32))
        factor = lax.rsqrt(lax.optimization_barrier(jnp.mean(gated * gated, axis=1, keepdims=True)) + 1e-05)
        result = (gated * factor * norm_gain).astype(jnp.bfloat16)
        new_state = jnp.exp(totals[0])[:, None, None] * carry + states[0]
        return (new_state, result)
    items = (head_inputs.reshape(blocks, SPAN, -1), gate_inputs.reshape(blocks, SPAN, -1), step_raw.reshape(blocks, SPAN, -1), state_write.reshape(blocks, SPAN, -1), state_read.reshape(blocks, SPAN, -1))
    start = jnp.zeros((HEADS, HEAD_DIM, STATE), jnp.float32)
    finish, outputs = lax.scan(advance, start, items)
    return outputs.reshape(SEQ, HEADS * HEAD_DIM)
```

```python
import functools
import math

import jax
import jax.numpy as jnp
from jax import lax
from jax.experimental import pallas as pl
from jax.experimental.pallas import tpu as pltpu
from jax.sharding import PartitionSpec as P

HEAD_DIM = 64
L = 128
LOG2E = math.log2(math.e)
F32 = jnp.float32
BF16 = jnp.bfloat16
MESH = pl.DeviceIdType.MESH
CAP = 100.0


def decays(raw_ref, rate_ref, pad_a, pad_s, heads):
    raw = raw_ref[...].astype(F32)
    step = jnp.maximum(raw, 0.0) + jnp.log1p(jnp.exp(-jnp.abs(raw)))
    pad_a[...] = jnp.zeros_like(pad_a)
    pad_s[...] = jnp.zeros_like(pad_s)
    pad_a[:, :heads] = -rate_ref[...] * step
    pad_s[:, :heads] = jnp.log2(step)
    row = lax.broadcasted_iota(jnp.int32, (L, L), 0)
    col = lax.broadcasted_iota(jnp.int32, (L, L), 1)
    tri = jnp.where(col <= row, 1.0, 0.0).astype(F32)
    run = jnp.dot(
        tri, pad_a[...], preferred_element_type=F32, precision=lax.Precision.HIGHEST
    )
    return run, run - pad_s[...]


def pair_lanes(cols, j, rows):
    lane = lax.broadcasted_iota(jnp.int32, (rows, L), 1)
    first = jnp.broadcast_to(cols[:, 2 * j : 2 * j + 1], (rows, L))
    second = jnp.broadcast_to(cols[:, 2 * j + 1 : 2 * j + 2], (rows, L))
    return jnp.where(lane < HEAD_DIM, first, second)


def state_kernel(
    heads, tiles, x_ref, raw_ref, rate_ref, write_ref,
    loc_ref, pre_ref, fin_ref, tot_ref, pad_a, pad_s, carry, total,
):
    chunk = pl.program_id(0)

    @pl.when(chunk == 0)
    def _():
        carry[...] = jnp.zeros_like(carry)
        total[...] = jnp.zeros_like(total)

    run, run_u = decays(raw_ref, rate_ref, pad_a, pad_s, heads)
    last = run[L - 1 : L, :]
    tail = jnp.exp2(last - run_u)
    write_t = write_ref[...].astype(F32).T.astype(BF16)
    pre_ref[0] = total[...]
    for j in range(tiles):
        x = x_ref[:, j * L : (j + 1) * L].astype(F32)
        weighted = (pair_lanes(tail, j, L) * x).astype(BF16)
        new = jnp.dot(write_t, weighted, preferred_element_type=F32)
        gone = pair_lanes(last, j, 1)
        old = carry[j]
        loc_ref[0, j] = old.astype(BF16)
        now = jnp.exp2(gone) * old + new
        carry[j] = now
        fin_ref[j] = now.astype(BF16)
        total[j : j + 1, :] = total[j : j + 1, :] + gone
    tot_ref[...] = total[...]


def exchange_kernel(
    count, tiles, group, fin_ref, tot_ref, out_ref,
    mate_buf, mate_tot, chain_in, chain_out,
    s_mate, r_mate, s_tot, r_tot, s_chain, r_chain,
):
    me = lax.axis_index("seq")
    odd = lax.rem(me, 2)
    pairs = count // 2
    place = me // 2
    mate = me + 1 - 2 * odd
    after = lax.rem(me + 2, count)
    before = lax.rem(me + count - 2, count)
    has_before = place > 0
    has_after = place < pairs - 1

    barrier = pltpu.get_barrier_semaphore()
    for other in (mate, after, before):
        pl.semaphore_signal(barrier, inc=1, device_id={"seq": other}, device_id_type=MESH)
    pl.semaphore_wait(barrier, 3)

    pieces = tiles // group

    def to_mate(p):
        part = pl.ds(p * group, group)
        return pltpu.make_async_remote_copy(
            src_ref=fin_ref.at[part], dst_ref=mate_buf.at[part],
            send_sem=s_mate.at[p], recv_sem=r_mate.at[p],
            device_id={"seq": mate}, device_id_type=MESH,
        )

    def to_next(p):
        part = pl.ds(p * group, group)
        return pltpu.make_async_remote_copy(
            src_ref=chain_out.at[part], dst_ref=chain_in.at[part],
            send_sem=s_chain.at[p], recv_sem=r_chain.at[p],
            device_id={"seq": after}, device_id_type=MESH,
        )

    tot_copy = pltpu.make_async_remote_copy(
        src_ref=tot_ref, dst_ref=mate_tot, send_sem=s_tot, recv_sem=r_tot,
        device_id={"seq": mate}, device_id_type=MESH,
    )
    tot_copy.start()
    for p in range(pieces):
        to_mate(p).start()

    @pl.when(jnp.logical_not(has_before))
    def _():
        chain_in[...] = jnp.zeros_like(chain_in)

    tot_copy.wait_recv()
    is_odd = odd == 1
    for p in range(pieces):
        to_mate(p).wait_recv()

        @pl.when(has_before)
        def _():
            to_next(p).wait_recv()

        for j in range(p * group, (p + 1) * group):
            own_tot = jnp.exp2(tot_ref[j : j + 1, :])
            other_tot = jnp.exp2(mate_tot[j : j + 1, :])
            own = fin_ref[j].astype(F32)
            other = mate_buf[j].astype(F32)
            coming = chain_in[j].astype(F32)
            early = jnp.where(is_odd, other, own)
            late = jnp.where(is_odd, own, other)
            early_tot = jnp.where(is_odd, other_tot, own_tot)
            late_tot = jnp.where(is_odd, own_tot, other_tot)
            middle = early_tot * coming + early
            chain_out[j] = (late_tot * middle + late).astype(BF16)
            out_ref[j] = jnp.where(is_odd, middle, coming)

        @pl.when(has_after)
        def _():
            to_next(p).start()

    tot_copy.wait_send()
    for p in range(pieces):
        to_mate(p).wait_send()

        @pl.when(has_after)
        def _():
            to_next(p).wait_send()


def output_kernel(
    heads, tiles, x_ref, z_ref, raw_ref, rate_ref, write_ref, read_ref,
    loc_ref, pre_ref, coming_ref, skip_ref,
    gated_ref, square_ref, pad_a, pad_s,
):
    run, run_u = decays(raw_ref, rate_ref, pad_a, pad_s, heads)
    run_rows = run_u.T
    grown = jnp.exp2(run)
    reads = read_ref[...]
    scores = lax.dot_general(
        reads, write_ref[...], (((1,), (1,)), ((), ())), preferred_element_type=F32
    )
    row = lax.broadcasted_iota(jnp.int32, (L, L), 0)
    col = lax.broadcasted_iota(jnp.int32, (L, L), 1)
    scores = jnp.where(col <= row, scores, 0.0)
    left = col < HEAD_DIM
    squares = jnp.zeros((L, L), F32)
    for j in range(tiles):
        x = x_ref[:, j * L : (j + 1) * L]
        mixes = []
        for k in (2 * j, 2 * j + 1):
            spread = run[:, k : k + 1] - run_rows[k : k + 1, :]
            mixes.append((scores * jnp.exp2(jnp.minimum(spread, CAP))).astype(BF16))
        wide = x.astype(F32)
        top = jnp.where(left, wide, 0.0).astype(BF16)
        bottom = jnp.where(left, 0.0, wide).astype(BF16)
        local = jnp.dot(
            jnp.concatenate(mixes, axis=1), jnp.concatenate([top, bottom], axis=0),
            preferred_element_type=F32,
        )
        entering = (
            loc_ref[0, j].astype(F32) + jnp.exp2(pre_ref[0, j : j + 1, :]) * coming_ref[j]
        ).astype(BF16)
        inter = jnp.dot(reads, entering, preferred_element_type=F32)
        y = local + skip_ref[j : j + 1, :] * wide + pair_lanes(grown, j, L) * inter
        z = z_ref[:, j * L : (j + 1) * L].astype(F32)
        gated = y * z * jax.nn.sigmoid(z)
        gated_ref[:, j * L : (j + 1) * L] = gated.astype(BF16)
        squares = squares + gated * gated
    square_ref[0] = jnp.sum(squares.T, axis=0, keepdims=True)


def on_device(
    count, head_inputs, gate_inputs, step_raw, decay_log, state_write, state_read, skip_gain, norm_gain
):
    tokens, inner = head_inputs.shape
    heads = inner // HEAD_DIM
    tiles = inner // L
    chunks = tokens // L
    states = state_write.shape[1]
    first = lax.axis_index("head") * heads
    rate = (LOG2E * jnp.exp(lax.dynamic_slice_in_dim(decay_log, first, heads))).reshape(1, heads)
    skips = lax.dynamic_slice_in_dim(skip_gain, first, heads)
    skips = jnp.broadcast_to(skips[:, None], (heads, HEAD_DIM)).reshape(tiles, L)
    gains = lax.dynamic_slice_in_dim(norm_gain, first * HEAD_DIM, inner)
    maps = lax.all_gather(
        jnp.concatenate([state_write, state_read], axis=1), "head", axis=0, tiled=True
    )
    group = math.gcd(tiles, 2)
    pieces = tiles // group
    sds = jax.ShapeDtypeStruct
    whole = lambda *shape: pl.BlockSpec(shape, lambda c: (0,) * len(shape))
    wide = pl.BlockSpec((L, inner), lambda c: (c, 0))
    raw_spec = pl.BlockSpec((L, heads), lambda c: (c, 0))
    write_spec = pl.BlockSpec((L, states), lambda c: (c, 0))
    read_spec = pl.BlockSpec((L, states), lambda c: (c, 1))
    loc_spec = pl.BlockSpec((1, tiles, states, L), lambda c: (c, 0, 0, 0))
    pre_spec = pl.BlockSpec((1, tiles, L), lambda c: (c, 0, 0))
    pads = [pltpu.VMEM((L, L), F32), pltpu.VMEM((L, L), F32)]

    loc, pre, fin, tot = pl.pallas_call(
        functools.partial(state_kernel, heads, tiles),
        grid=(chunks,),
        in_specs=[wide, raw_spec, whole(1, heads), write_spec],
        out_specs=[loc_spec, pre_spec, whole(tiles, states, L), whole(tiles, L)],
        out_shape=[
            sds((chunks, tiles, states, L), BF16),
            sds((chunks, tiles, L), F32),
            sds((tiles, states, L), BF16),
            sds((tiles, L), F32),
        ],
        scratch_shapes=pads + [pltpu.VMEM((tiles, states, L), F32), pltpu.VMEM((tiles, L), F32)],
        name="states",
    )(head_inputs, step_raw, rate, maps)

    vmem = pl.BlockSpec(memory_space=pltpu.VMEM)
    buf = pltpu.VMEM((tiles, states, L), BF16)
    sems = pltpu.SemaphoreType.DMA((pieces,))
    coming = pl.pallas_call(
        functools.partial(exchange_kernel, count, tiles, group),
        in_specs=[vmem, vmem],
        out_specs=vmem,
        out_shape=sds((tiles, states, L), F32),
        scratch_shapes=[
            buf, pltpu.VMEM((tiles, L), F32), buf, buf,
            sems, sems, pltpu.SemaphoreType.DMA, pltpu.SemaphoreType.DMA, sems, sems,
        ],
        compiler_params=pltpu.CompilerParams(collective_id=0, has_side_effects=True),
        name="exchange",
    )(fin, tot)

    gated, squares = pl.pallas_call(
        functools.partial(output_kernel, heads, tiles),
        grid=(chunks,),
        in_specs=[
            wide, wide, raw_spec, whole(1, heads), write_spec, read_spec,
            loc_spec, pre_spec, whole(tiles, states, L), whole(tiles, L),
        ],
        out_specs=[wide, pl.BlockSpec((1, 1, L), lambda c: (c, 0, 0))],
        out_shape=[sds((tokens, inner), BF16), sds((chunks, 1, L), F32)],
        scratch_shapes=pads,
        name="outputs",
    )(head_inputs, gate_inputs, step_raw, rate, maps, maps, loc, pre, coming, skips)

    squares = lax.psum(squares, "head")
    factor = lax.rsqrt(squares.reshape(tokens, 1) / norm_gain.shape[0] + 1e-05)
    return (gated.astype(F32) * factor * gains).astype(BF16)


def solution(mesh):
    return jax.shard_map(
        functools.partial(on_device, mesh.shape["seq"]),
        mesh=mesh,
        in_specs=(
            P("seq", "head"),
            P("seq", "head"),
            P("seq", "head"),
            P(),
            P(("seq", "head"), None),
            P(("seq", "head"), None),
            P(),
            P(),
        ),
        out_specs=P("seq", "head"),
        check_vma=False,
    )
```

```python
import functools
import math

import jax
import jax.numpy as jnp
from jax import lax
from jax.experimental import pallas as pl
from jax.experimental.pallas import tpu as pltpu
from jax.sharding import PartitionSpec as P

HEAD_DIM = 64
L = 128
SLOT = 32
LOG2E = math.log2(math.e)
F32 = jnp.float32
BF16 = jnp.bfloat16
MESH = pl.DeviceIdType.MESH
CAP = 100.0


def pair_lanes(first, second, rows):
    lane = lax.broadcasted_iota(jnp.int32, (rows, L), 1)
    first = jnp.broadcast_to(first, (rows, L))
    second = jnp.broadcast_to(second, (rows, L))
    return jnp.where(lane < HEAD_DIM, first, second)


def layer_kernel(
    count, peers, heads, tiles, group, chunks,
    x_hbm, z_hbm, raw_ref, decay_ref, write_ref, read_ref, skip_ref, gain_ref,
    gated_ref, square_ref,
    x_ref, z_ref, writes, reads, sums, run_rows, cols, masked, local,
    loc, pre, fin, carry, tot, mate_buf, mate_tot, chain_in, chain_out, coming_ref,
    spot, sq, sq_own, sq_in,
    x_sem, z_sem, s_w, r_w, s_r, r_r, s_mate, r_mate, s_tot, r_tot, s_chain, r_chain, s_sq, r_sq,
):
    me = lax.axis_index("seq")
    head = lax.axis_index("head")
    odd = lax.rem(me, 2)
    is_odd = odd == 1
    pairs = count // 2
    place = me // 2
    mate = me + 1 - 2 * odd
    after = lax.rem(me + 2, count)
    before = lax.rem(me + count - 2, count)
    has_before = place > 0
    has_after = place < pairs - 1
    pieces = tiles // group
    width = group * L
    rows = write_ref.shape[0]

    def load_x(p):
        span = pl.ds(p * width, width)
        return pltpu.make_async_copy(x_hbm.at[:, span], x_ref.at[:, span], x_sem.at[p])

    load_z = pltpu.make_async_copy(z_hbm, z_ref, z_sem)
    for p in range(pieces):
        load_x(p).start()
    load_z.start()

    barrier = pltpu.get_barrier_semaphore()
    for other in (mate, after, before):
        pl.semaphore_signal(barrier, inc=1, device_id={"seq": other}, device_id_type=MESH)
    for d in range(1, peers):
        pl.semaphore_signal(
            barrier, inc=1, device_id={"head": lax.rem(head + d, peers)}, device_id_type=MESH
        )
    pl.semaphore_wait(barrier, 3 + peers - 1)

    def to_peer(src, dst, send, recv, d):
        return pltpu.make_async_remote_copy(
            src_ref=src, dst_ref=dst, send_sem=send.at[d - 1], recv_sem=recv.at[d - 1],
            device_id={"head": lax.rem(head + d, peers)}, device_id_type=MESH,
        )

    own_rows = pl.ds(pl.multiple_of(head * rows, L), rows)
    give_w = [to_peer(write_ref, writes.at[own_rows], s_w, r_w, d) for d in range(1, peers)]
    give_r = [to_peer(read_ref, reads.at[own_rows], s_r, r_r, d) for d in range(1, peers)]
    for copy in give_w + give_r:
        copy.start()
    writes[own_rows, :] = write_ref[...]
    reads[own_rows, :] = read_ref[...]

    total_heads = decay_ref.shape[1]
    spot[...] = jnp.zeros_like(spot)
    spot[0:1, :total_heads] = decay_ref[...]
    spot[1:2, :total_heads] = skip_ref[...]
    rolled = pltpu.roll(spot[...], lax.rem(L - head * heads, L), 1)
    skip_row = rolled[1:2, :]
    square = jnp.broadcast_to(rolled[0:1, :], (L, L)).T
    rate = jnp.exp(square[:heads, :1]) * LOG2E
    raw = raw_ref[...].astype(F32)
    step = jnp.maximum(raw, 0.0) + jnp.log1p(jnp.exp(-jnp.abs(raw)))
    falls = -rate * step
    steps = jnp.log2(step)
    sums[...] = jnp.zeros_like(sums)
    for c in range(chunks):
        sums[c, :heads, :] = falls[:, c * L : (c + 1) * L]
    row = lax.broadcasted_iota(jnp.int32, (L, L), 0)
    col = lax.broadcasted_iota(jnp.int32, (L, L), 1)
    upper = jnp.where(row <= col, 1.0, 0.0).astype(F32)
    run_all = jnp.dot(
        sums[...].reshape(chunks * SLOT, L), upper,
        preferred_element_type=F32, precision=lax.Precision.HIGHEST,
    ).reshape(chunks, SLOT, L)
    sums[:, :, :] = jnp.zeros_like(sums)
    for c in range(chunks):
        sums[c, :heads, :] = steps[:, c * L : (c + 1) * L]
    tot[...] = jnp.zeros_like(tot)
    for c in range(chunks):
        run = run_all[c]
        run_u = run - sums[c]
        run_rows[c] = run_u
        last = jnp.broadcast_to(run[:, L - 1 : L], (SLOT, L))
        cols[c] = jnp.concatenate(
            [run, jnp.exp2(run), jnp.exp2(last - run_u), last], axis=0
        ).T
        pre[c] = tot[...]
        for j in range(tiles):
            at = 3 * SLOT + 2 * j
            gone = pair_lanes(cols[c, 0:1, at : at + 1], cols[c, 0:1, at + 1 : at + 2], 1)
            tot[j : j + 1, :] = tot[j : j + 1, :] + gone

    tot_copy = pltpu.make_async_remote_copy(
        src_ref=tot, dst_ref=mate_tot, send_sem=s_tot, recv_sem=r_tot,
        device_id={"seq": mate}, device_id_type=MESH,
    )
    tot_copy.start()
    for copy in give_w:
        copy.wait_recv()

    def to_mate(p):
        part = pl.ds(p * group, group)
        return pltpu.make_async_remote_copy(
            src_ref=fin.at[part], dst_ref=mate_buf.at[part],
            send_sem=s_mate.at[p], recv_sem=r_mate.at[p],
            device_id={"seq": mate}, device_id_type=MESH,
        )

    def to_next(p):
        part = pl.ds(p * group, group)
        return pltpu.make_async_remote_copy(
            src_ref=chain_out.at[part], dst_ref=chain_in.at[part],
            send_sem=s_chain.at[p], recv_sem=r_chain.at[p],
            device_id={"seq": after}, device_id_type=MESH,
        )

    def at_chunk(c):
        return pl.ds(pl.multiple_of(c * L, L), L)

    for p in range(pieces):
        load_x(p).wait()
        carry[...] = jnp.zeros_like(carry)

        def advance(c, _, p=p):
            here = at_chunk(c)
            tail = cols[c]
            weighted = []
            for j in range(p * group, (p + 1) * group):
                at = 2 * SLOT + 2 * j
                wide = pair_lanes(tail[:, at : at + 1], tail[:, at + 1 : at + 2], L)
                x = x_ref[here, j * L : (j + 1) * L].astype(F32)
                weighted.append((wide * x).astype(BF16))
            new = lax.dot_general(
                writes[here, :], jnp.concatenate(weighted, axis=1),
                (((0,), (0,)), ((), ())), preferred_element_type=F32,
            )
            for i in range(group):
                j = p * group + i
                at = 3 * SLOT + 2 * j
                gone = pair_lanes(tail[0:1, at : at + 1], tail[0:1, at + 1 : at + 2], 1)
                old = carry[i]
                loc[c, j] = old.astype(BF16)
                carry[i] = jnp.exp2(gone) * old + new[:, i * L : (i + 1) * L]
            return 0

        lax.fori_loop(0, chunks, advance, 0, unroll=2)
        for i in range(group):
            fin[p * group + i] = carry[i].astype(BF16)
        to_mate(p).start()

    @pl.when(jnp.logical_not(has_before))
    def _():
        chain_in[...] = jnp.zeros_like(chain_in)

    for copy in give_r:
        copy.wait_recv()

    def score(c, _):
        here = at_chunk(c)
        scores = lax.dot_general(
            reads[here, :], writes[here, :], (((1,), (1,)), ((), ())),
            preferred_element_type=F32,
        )
        masked[c] = jnp.where(col <= row, scores, 0.0)
        return 0

    lax.fori_loop(0, chunks, score, 0)
    tot_copy.wait_recv()

    def chain_step(p):
        to_mate(p).wait_recv()

        @pl.when(has_before)
        def _():
            to_next(p).wait_recv()

        for i in range(group):
            j = p * group + i
            own_tot = jnp.exp2(tot[pl.ds(j, 1), :])
            other_tot = jnp.exp2(mate_tot[pl.ds(j, 1), :])
            own = fin[j].astype(F32)
            other = mate_buf[j].astype(F32)
            coming = chain_in[j].astype(F32)
            early = jnp.where(is_odd, other, own)
            late = jnp.where(is_odd, own, other)
            early_tot = jnp.where(is_odd, other_tot, own_tot)
            late_tot = jnp.where(is_odd, own_tot, other_tot)
            middle = early_tot * coming + early
            chain_out[j] = (late_tot * middle + late).astype(BF16)
            coming_ref[j] = jnp.where(is_odd, middle, coming)

        @pl.when(has_after)
        def _():
            to_next(p).start()

    shift = jnp.minimum(place, pieces)
    left = col < HEAD_DIM
    for k in range(pieces):
        due = k - shift

        @pl.when(due >= 0)
        def _():
            chain_step(due)

        def inside(c, _, p=k):
            here = at_chunk(c)
            run = cols[c]
            scores = masked[c]
            for j in range(p * group, (p + 1) * group):
                x = x_ref[here, j * L : (j + 1) * L].astype(F32)
                mixes = []
                for h in (2 * j, 2 * j + 1):
                    spread = run[:, h : h + 1] - run_rows[c, h : h + 1, :]
                    mixes.append((scores * jnp.exp2(jnp.minimum(spread, CAP))).astype(BF16))
                top = jnp.where(left, x, 0.0).astype(BF16)
                bottom = jnp.where(left, 0.0, x).astype(BF16)
                skip = pair_lanes(
                    skip_row[:, 2 * j : 2 * j + 1], skip_row[:, 2 * j + 1 : 2 * j + 2], 1
                )
                local[here, j * L : (j + 1) * L] = skip * x + jnp.dot(
                    jnp.concatenate(mixes, axis=1), jnp.concatenate([top, bottom], axis=0),
                    preferred_element_type=F32,
                )
            return 0

        lax.fori_loop(0, chunks, inside, 0)

    load_z.wait()
    sq[...] = jnp.zeros_like(sq)
    first_gain = pl.multiple_of(head * (tiles * L), L)
    for k in range(pieces):

        @pl.when(k >= pieces - shift)
        def _():
            chain_step(jnp.int32(k))

        gain = gain_ref[:, pl.ds(first_gain + k * width, width)]

        def finish(c, _, p=k, gain=gain):
            here = at_chunk(c)
            grown = cols[c]
            entering = []
            for j in range(p * group, (p + 1) * group):
                entering.append(
                    (
                        loc[c, j].astype(F32) + jnp.exp2(pre[c, j : j + 1, :]) * coming_ref[j]
                    ).astype(BF16)
                )
            inter = jnp.dot(
                reads[here, :], jnp.concatenate(entering, axis=1), preferred_element_type=F32
            )
            squares = sq[c]
            for i in range(group):
                j = p * group + i
                at = SLOT + 2 * j
                span = slice(j * L, (j + 1) * L)
                y = local[here, span] + (
                    pair_lanes(grown[:, at : at + 1], grown[:, at + 1 : at + 2], L)
                    * inter[:, i * L : (i + 1) * L]
                )
                z = z_ref[here, span].astype(F32)
                gated = y * z * jax.nn.sigmoid(z)
                squares = squares + gated * gated
                gated_ref[here, span] = (gated * gain[:, i * L : (i + 1) * L]).astype(BF16)
            sq[c] = squares
            return 0

        lax.fori_loop(0, chunks, finish, 0)

    for c in range(chunks):
        sq_own[c : c + 1, :] = jnp.sum(sq[c].T, axis=0, keepdims=True)
    give_sq = [to_peer(sq_own, sq_in.at[d - 1], s_sq, r_sq, d) for d in range(1, peers)]
    for copy in give_sq:
        copy.start()
    square_sum = sq_own[...]
    for d in range(1, peers):
        give_sq[d - 1].wait_recv()
        square_sum = square_sum + sq_in[d - 1]
    square_ref[...] = square_sum

    tot_copy.wait_send()
    for copy in give_w + give_r + give_sq:
        copy.wait_send()
    for p in range(pieces):
        to_mate(p).wait_send()

        @pl.when(has_after)
        def _():
            to_next(p).wait_send()


def scale_kernel(part, channels, gated_ref, square_ref, out_ref):
    i = pl.program_id(0)
    for k in range(part):
        sums = square_ref[pl.ds(i * part + k, 1), :]
        factor = lax.rsqrt(jnp.broadcast_to(sums, (L, L)).T / channels + 1e-05)
        here = slice(k * L, (k + 1) * L)
        for j in range(gated_ref.shape[1] // L):
            span = slice(j * L, (j + 1) * L)
            out_ref[here, span] = (gated_ref[here, span].astype(F32) * factor).astype(BF16)


def on_device(
    count, peers, head_inputs, gate_inputs, step_raw, decay_log, state_write, state_read, skip_gain, norm_gain
):
    tokens, inner = head_inputs.shape
    heads = inner // HEAD_DIM
    tiles = inner // L
    chunks = tokens // L
    states = state_write.shape[1]
    group = math.gcd(tiles, 2)
    pieces = tiles // group
    sds = jax.ShapeDtypeStruct
    vmem = pl.BlockSpec(memory_space=pltpu.VMEM)
    hbm = pl.BlockSpec(memory_space=pl.ANY)
    dma = pltpu.SemaphoreType.DMA
    state = (tiles, states, L)
    gated, squares = pl.pallas_call(
        functools.partial(layer_kernel, count, peers, heads, tiles, group, chunks),
        in_specs=[hbm, hbm] + [vmem] * 6,
        out_specs=[vmem, vmem],
        out_shape=[sds((tokens, inner), BF16), sds((chunks, L), F32)],
        scratch_shapes=[
            pltpu.VMEM((tokens, inner), BF16),
            pltpu.VMEM((tokens, inner), BF16),
            pltpu.VMEM((tokens, states), BF16),
            pltpu.VMEM((tokens, states), BF16),
            pltpu.VMEM((chunks, SLOT, L), F32),
            pltpu.VMEM((chunks, SLOT, L), F32),
            pltpu.VMEM((chunks, L, L), F32),
            pltpu.VMEM((chunks, L, L), F32),
            pltpu.VMEM((tokens, inner), F32),
            pltpu.VMEM((chunks,) + state, BF16),
            pltpu.VMEM((chunks, tiles, L), F32),
            pltpu.VMEM(state, BF16),
            pltpu.VMEM((group, states, L), F32),
            pltpu.VMEM((tiles, L), F32),
            pltpu.VMEM(state, BF16),
            pltpu.VMEM((tiles, L), F32),
            pltpu.VMEM(state, BF16),
            pltpu.VMEM(state, BF16),
            pltpu.VMEM(state, F32),
            pltpu.VMEM((8, L), F32),
            pltpu.VMEM((chunks, L, L), F32),
            pltpu.VMEM((chunks, L), F32),
            pltpu.VMEM((peers - 1, chunks, L), F32),
            dma((pieces,)), dma,
            dma((peers - 1,)), dma((peers - 1,)), dma((peers - 1,)), dma((peers - 1,)),
            dma((pieces,)), dma((pieces,)), dma, dma, dma((pieces,)), dma((pieces,)),
            dma((peers - 1,)), dma((peers - 1,)),
        ],
        compiler_params=pltpu.CompilerParams(
            collective_id=0, has_side_effects=True, vmem_limit_bytes=50 * 2**20
        ),
        name="layer",
    )(
        head_inputs, gate_inputs, step_raw.T, decay_log.reshape(1, -1),
        state_write, state_read, skip_gain.reshape(1, -1), norm_gain.reshape(1, -1),
    )
    part = 2
    wide = pl.BlockSpec((part * L, inner), lambda c: (c, 0))
    return pl.pallas_call(
        functools.partial(scale_kernel, part, norm_gain.shape[0]),
        grid=(chunks // part,),
        in_specs=[wide, pl.BlockSpec((chunks, L), lambda c: (0, 0))],
        out_specs=wide,
        out_shape=sds((tokens, inner), BF16),
        name="scale",
    )(gated, squares)


def solution(mesh):
    return jax.shard_map(
        functools.partial(on_device, mesh.shape["seq"], mesh.shape["head"]),
        mesh=mesh,
        in_specs=(
            P("seq", "head"),
            P("seq", "head"),
            P("seq", "head"),
            P(),
            P(("seq", "head"), None),
            P(("seq", "head"), None),
            P(),
            P(),
        ),
        out_specs=P("seq", "head"),
        check_vma=False,
    )
```

```python
import functools
import math

import jax
import jax.numpy as jnp
from jax import lax
from jax.experimental import pallas as pl
from jax.experimental.pallas import tpu as pltpu
from jax.sharding import PartitionSpec as P

HEAD_DIM = 64
L = 128
SLOT = 32
LOG2E = math.log2(math.e)
F32 = jnp.float32
BF16 = jnp.bfloat16
MESH = pl.DeviceIdType.MESH
CAP = 100.0
UNROLL = 4
LEAD = 3
HOP = 2


def pair_lanes(first, second, rows):
    lane = lax.broadcasted_iota(jnp.int32, (rows, L), 1)
    first = jnp.broadcast_to(first, (rows, L))
    second = jnp.broadcast_to(second, (rows, L))
    return jnp.where(lane < HEAD_DIM, first, second)


def layer_kernel(
    count, peers, heads, tiles, group, chunks,
    x_hbm, z_hbm, raw_hbm, decay_hbm, write_hbm, read_hbm, skip_hbm, gain_hbm,
    gated_hbm, square_ref, gated_ref, out_sem, raw_ref, decay_ref, skip_ref, gain_ref, writes_t,
    x_ref, z_ref, writes, reads, sums, run_rows, cols, masked, local,
    loc, pre, fin, carry, tot, mate_buf, mate_tot, chain_in, chain_out, coming_ref,
    spot, sq, sq_own, sq_in,
    x_sem, z_sem, in_sem, s_w, r_w, s_r, r_r, s_mate, r_mate, s_tot, r_tot, s_chain, r_chain, s_sq, r_sq,
):
    me = lax.axis_index("seq")
    head = lax.axis_index("head")
    odd = lax.rem(me, 2)
    is_odd = odd == 1
    pairs = count // 2
    place = me // 2
    mate = me + 1 - 2 * odd
    after = lax.rem(me + 2, count)
    before = lax.rem(me + count - 2, count)
    has_before = place > 0
    has_after = place < pairs - 1
    pieces = tiles // group
    width = group * L
    rows = write_hbm.shape[0]
    own_rows = pl.ds(pl.multiple_of(head * rows, L), rows)
    inputs = [
        pltpu.make_async_copy(source, target, in_sem.at[i])
        for i, (source, target) in enumerate(
            [
                (write_hbm, writes.at[own_rows]),
                (read_hbm, reads.at[own_rows]),
                (raw_hbm, raw_ref),
                (decay_hbm, decay_ref),
                (skip_hbm, skip_ref),
                (gain_hbm, gain_ref),
            ]
        )
    ]
    for copy in inputs:
        copy.start()

    def load_x(p):
        span = pl.ds(p * width, width)
        return pltpu.make_async_copy(x_hbm.at[:, span], x_ref.at[:, span], x_sem.at[p])

    def store(p):
        span = pl.ds(p * width, width)
        return pltpu.make_async_copy(
            gated_ref.at[:, span], gated_hbm.at[:, span], out_sem.at[p]
        )

    load_z = pltpu.make_async_copy(z_hbm, z_ref, z_sem)
    for p in range(pieces):
        load_x(p).start()
    load_z.start()

    barrier = pltpu.get_barrier_semaphore()
    for other in (mate, after, before):
        pl.semaphore_signal(barrier, inc=1, device_id={"seq": other}, device_id_type=MESH)
    for d in range(1, peers):
        pl.semaphore_signal(
            barrier, inc=1, device_id={"head": lax.rem(head + d, peers)}, device_id_type=MESH
        )
    pl.semaphore_wait(barrier, 3 + peers - 1)

    def to_peer(src, dst, send, recv, d):
        return pltpu.make_async_remote_copy(
            src_ref=src, dst_ref=dst, send_sem=send.at[d - 1], recv_sem=recv.at[d - 1],
            device_id={"head": lax.rem(head + d, peers)}, device_id_type=MESH,
        )

    give_w = [to_peer(writes.at[own_rows], writes.at[own_rows], s_w, r_w, d) for d in range(1, peers)]
    give_r = [to_peer(reads.at[own_rows], reads.at[own_rows], s_r, r_r, d) for d in range(1, peers)]
    inputs[0].wait()
    for copy in give_w:
        copy.start()
    inputs[1].wait()
    for copy in give_r:
        copy.start()
    for copy in inputs[2:]:
        copy.wait()

    total_heads = decay_ref.shape[1]
    spot[...] = jnp.zeros_like(spot)
    spot[0:1, :total_heads] = decay_ref[...]
    spot[1:2, :total_heads] = skip_ref[...]
    rolled = pltpu.roll(spot[...], lax.rem(L - head * heads, L), 1)
    skip_row = rolled[1:2, :]
    square = jnp.broadcast_to(rolled[0:1, :], (L, L)).T
    rate = jnp.exp(square[:heads, :1]) * LOG2E
    raw = raw_ref[...].astype(F32)
    step = jnp.maximum(raw, 0.0) + jnp.log1p(jnp.exp(-jnp.abs(raw)))
    falls = -rate * step
    steps = jnp.log2(step)
    sums[...] = jnp.zeros_like(sums)
    for c in range(chunks):
        sums[c, :heads, :] = falls[:, c * L : (c + 1) * L]
    row = lax.broadcasted_iota(jnp.int32, (L, L), 0)
    col = lax.broadcasted_iota(jnp.int32, (L, L), 1)
    upper = jnp.where(row <= col, 1.0, 0.0).astype(F32)
    run_all = jnp.dot(
        sums[...].reshape(chunks * SLOT, L), upper,
        preferred_element_type=F32, precision=lax.Precision.HIGHEST,
    ).reshape(chunks, SLOT, L)
    sums[:, :, :] = jnp.zeros_like(sums)
    for c in range(chunks):
        sums[c, :heads, :] = steps[:, c * L : (c + 1) * L]
    tot[...] = jnp.zeros_like(tot)
    for c in range(chunks):
        run = run_all[c]
        run_u = run - sums[c]
        run_rows[c] = run_u
        last = jnp.broadcast_to(run[:, L - 1 : L], (SLOT, L))
        cols[c] = jnp.concatenate(
            [run, jnp.exp2(run), jnp.exp2(last - run_u), last], axis=0
        ).T
        pre[c] = tot[...]
        for j in range(tiles):
            at = 3 * SLOT + 2 * j
            gone = pair_lanes(cols[c, 0:1, at : at + 1], cols[c, 0:1, at + 1 : at + 2], 1)
            tot[j : j + 1, :] = tot[j : j + 1, :] + gone

    tot_copy = pltpu.make_async_remote_copy(
        src_ref=tot, dst_ref=mate_tot, send_sem=s_tot, recv_sem=r_tot,
        device_id={"seq": mate}, device_id_type=MESH,
    )
    tot_copy.start()
    for copy in give_w:
        copy.wait_recv()
    for c in range(chunks):
        writes_t[c] = writes[c * L : (c + 1) * L, :].astype(F32).T.astype(BF16)

    def to_mate(p):
        part = pl.ds(p * group, group)
        return pltpu.make_async_remote_copy(
            src_ref=fin.at[part], dst_ref=mate_buf.at[part],
            send_sem=s_mate.at[p], recv_sem=r_mate.at[p],
            device_id={"seq": mate}, device_id_type=MESH,
        )

    def to_next(p):
        part = pl.ds(p * group, group)
        return pltpu.make_async_remote_copy(
            src_ref=chain_out.at[part], dst_ref=chain_in.at[part],
            send_sem=s_chain.at[p], recv_sem=r_chain.at[p],
            device_id={"seq": after}, device_id_type=MESH,
        )

    def at_chunk(c):
        return pl.ds(pl.multiple_of(c * L, L), L)

    def chain_step(p):
        to_mate(p).wait_recv()

        @pl.when(has_before)
        def _():
            to_next(p).wait_recv()

        for i in range(group):
            j = p * group + i
            own_tot = jnp.exp2(tot[pl.ds(j, 1), :])
            other_tot = jnp.exp2(mate_tot[pl.ds(j, 1), :])
            own = fin[j].astype(F32)
            other = mate_buf[j].astype(F32)
            coming = chain_in[j].astype(F32)
            early = jnp.where(is_odd, other, own)
            late = jnp.where(is_odd, own, other)
            early_tot = jnp.where(is_odd, other_tot, own_tot)
            late_tot = jnp.where(is_odd, own_tot, other_tot)
            middle = early_tot * coming + early
            chain_out[j] = (late_tot * middle + late).astype(BF16)
            coming_ref[j] = jnp.where(is_odd, middle, coming)

        @pl.when(has_after)
        def _():
            to_next(p).start()

    def maybe_step(slot):
        due = slot - shift

        @pl.when(jnp.logical_and(due >= 0, due < pieces))
        def _():
            chain_step(due)

    lead = min(LEAD, pieces)
    shift = jnp.minimum(lead + HOP * place, 2 * pieces)

    @pl.when(jnp.logical_not(has_before))
    def _():
        chain_in[...] = jnp.zeros_like(chain_in)

    for p in range(pieces):
        if p == lead:
            tot_copy.wait_recv()
        if p >= lead:
            maybe_step(p)
        load_x(p).wait()
        carry[...] = jnp.zeros_like(carry)

        def advance(c, _, p=p):
            here = at_chunk(c)
            tail = cols[c]
            weighted = []
            for j in range(p * group, (p + 1) * group):
                at = 2 * SLOT + 2 * j
                wide = pair_lanes(tail[:, at : at + 1], tail[:, at + 1 : at + 2], L)
                x = x_ref[here, j * L : (j + 1) * L].astype(F32)
                weighted.append((wide * x).astype(BF16))
            new = jnp.dot(
                writes_t[c], jnp.concatenate(weighted, axis=1), preferred_element_type=F32
            )
            for i in range(group):
                j = p * group + i
                at = 3 * SLOT + 2 * j
                gone = pair_lanes(tail[0:1, at : at + 1], tail[0:1, at + 1 : at + 2], 1)
                old = carry[i]
                loc[c, j] = old.astype(BF16)
                carry[i] = jnp.exp2(gone) * old + new[:, i * L : (i + 1) * L]
            return 0

        lax.fori_loop(0, chunks, advance, 0, unroll=UNROLL)
        for i in range(group):
            fin[p * group + i] = carry[i].astype(BF16)
        to_mate(p).start()

    if lead >= pieces:
        tot_copy.wait_recv()
    for copy in give_r:
        copy.wait_recv()

    def score(c, _):
        here = at_chunk(c)
        scores = lax.dot_general(
            reads[here, :], writes[here, :], (((1,), (1,)), ((), ())),
            preferred_element_type=F32,
        )
        masked[c] = jnp.where(col <= row, scores, 0.0)
        return 0

    lax.fori_loop(0, chunks, score, 0, unroll=UNROLL)
    left = col < HEAD_DIM
    for k in range(pieces):
        maybe_step(pieces + k)

        def inside(c, _, p=k):
            here = at_chunk(c)
            run = cols[c]
            scores = masked[c]
            for j in range(p * group, (p + 1) * group):
                x = x_ref[here, j * L : (j + 1) * L].astype(F32)
                mixes = []
                for h in (2 * j, 2 * j + 1):
                    spread = run[:, h : h + 1] - run_rows[c, h : h + 1, :]
                    mixes.append((scores * jnp.exp2(jnp.minimum(spread, CAP))).astype(BF16))
                top = jnp.where(left, x, 0.0).astype(BF16)
                bottom = jnp.where(left, 0.0, x).astype(BF16)
                skip = pair_lanes(
                    skip_row[:, 2 * j : 2 * j + 1], skip_row[:, 2 * j + 1 : 2 * j + 2], 1
                )
                local[here, j * L : (j + 1) * L] = skip * x + jnp.dot(
                    jnp.concatenate(mixes, axis=1), jnp.concatenate([top, bottom], axis=0),
                    preferred_element_type=F32,
                )
            return 0

        lax.fori_loop(0, chunks, inside, 0, unroll=UNROLL)

    load_z.wait()
    sq[...] = jnp.zeros_like(sq)
    first_gain = pl.multiple_of(head * (tiles * L), L)
    for k in range(pieces):

        @pl.when(k + shift >= 2 * pieces)
        def _():
            chain_step(jnp.int32(k))

        gain = gain_ref[:, pl.ds(first_gain + k * width, width)]

        def finish(c, _, p=k, gain=gain):
            here = at_chunk(c)
            grown = cols[c]
            entering = []
            for j in range(p * group, (p + 1) * group):
                entering.append(
                    (
                        loc[c, j].astype(F32) + jnp.exp2(pre[c, j : j + 1, :]) * coming_ref[j]
                    ).astype(BF16)
                )
            inter = jnp.dot(
                reads[here, :], jnp.concatenate(entering, axis=1), preferred_element_type=F32
            )
            squares = sq[c]
            for i in range(group):
                j = p * group + i
                at = SLOT + 2 * j
                span = slice(j * L, (j + 1) * L)
                y = local[here, span] + (
                    pair_lanes(grown[:, at : at + 1], grown[:, at + 1 : at + 2], L)
                    * inter[:, i * L : (i + 1) * L]
                )
                z = z_ref[here, span].astype(F32)
                gated = y * z * jax.nn.sigmoid(z)
                squares = squares + gated * gated
                gated_ref[here, span] = (gated * gain[:, i * L : (i + 1) * L]).astype(BF16)
            sq[c] = squares
            return 0

        lax.fori_loop(0, chunks, finish, 0, unroll=UNROLL)
        store(k).start()

    for c in range(chunks):
        sq_own[c : c + 1, :] = jnp.sum(sq[c].T, axis=0, keepdims=True)
    give_sq = [to_peer(sq_own, sq_in.at[d - 1], s_sq, r_sq, d) for d in range(1, peers)]
    for copy in give_sq:
        copy.start()
    square_sum = sq_own[...]
    for d in range(1, peers):
        give_sq[d - 1].wait_recv()
        square_sum = square_sum + sq_in[d - 1]
    square_ref[...] = square_sum

    tot_copy.wait_send()
    for copy in give_w + give_r + give_sq:
        copy.wait_send()
    for p in range(pieces):
        store(p).wait()
        to_mate(p).wait_send()

        @pl.when(has_after)
        def _():
            to_next(p).wait_send()


def scale_kernel(part, channels, gated_ref, square_ref, out_ref):
    i = pl.program_id(0)
    for k in range(part):
        sums = square_ref[pl.ds(i * part + k, 1), :]
        factor = lax.rsqrt(jnp.broadcast_to(sums, (L, L)).T / channels + 1e-05)
        here = slice(k * L, (k + 1) * L)
        for j in range(gated_ref.shape[1] // L):
            span = slice(j * L, (j + 1) * L)
            out_ref[here, span] = (gated_ref[here, span].astype(F32) * factor).astype(BF16)


def on_device(
    count, peers, head_inputs, gate_inputs, step_raw, decay_log, state_write, state_read, skip_gain, norm_gain
):
    tokens, inner = head_inputs.shape
    heads = inner // HEAD_DIM
    tiles = inner // L
    chunks = tokens // L
    states = state_write.shape[1]
    group = math.gcd(tiles, 2)
    pieces = tiles // group
    sds = jax.ShapeDtypeStruct
    vmem = pl.BlockSpec(memory_space=pltpu.VMEM)
    hbm = pl.BlockSpec(memory_space=pltpu.HBM)
    dma = pltpu.SemaphoreType.DMA
    state = (tiles, states, L)
    gated, squares = pl.pallas_call(
        functools.partial(layer_kernel, count, peers, heads, tiles, group, chunks),
        in_specs=[hbm] * 8,
        out_specs=[hbm, vmem],
        out_shape=[sds((tokens, inner), BF16), sds((chunks, L), F32)],
        scratch_shapes=[
            pltpu.VMEM((tokens, inner), BF16),
            dma((pieces,)),
            pltpu.VMEM((heads, tokens), BF16),
            pltpu.VMEM((1, decay_log.shape[0]), F32),
            pltpu.VMEM((1, skip_gain.shape[0]), F32),
            pltpu.VMEM((1, norm_gain.shape[0]), F32),
            pltpu.VMEM((chunks, states, L), BF16),
            pltpu.VMEM((tokens, inner), BF16),
            pltpu.VMEM((tokens, inner), BF16),
            pltpu.VMEM((tokens, states), BF16),
            pltpu.VMEM((tokens, states), BF16),
            pltpu.VMEM((chunks, SLOT, L), F32),
            pltpu.VMEM((chunks, SLOT, L), F32),
            pltpu.VMEM((chunks, L, L), F32),
            pltpu.VMEM((chunks, L, L), F32),
            pltpu.VMEM((tokens, inner), F32),
            pltpu.VMEM((chunks,) + state, BF16),
            pltpu.VMEM((chunks, tiles, L), F32),
            pltpu.VMEM(state, BF16),
            pltpu.VMEM((group, states, L), F32),
            pltpu.VMEM((tiles, L), F32),
            pltpu.VMEM(state, BF16),
            pltpu.VMEM((tiles, L), F32),
            pltpu.VMEM(state, BF16),
            pltpu.VMEM(state, BF16),
            pltpu.VMEM(state, F32),
            pltpu.VMEM((8, L), F32),
            pltpu.VMEM((chunks, L, L), F32),
            pltpu.VMEM((chunks, L), F32),
            pltpu.VMEM((peers - 1, chunks, L), F32),
            dma((pieces,)), dma, dma((6,)),
            dma((peers - 1,)), dma((peers - 1,)), dma((peers - 1,)), dma((peers - 1,)),
            dma((pieces,)), dma((pieces,)), dma, dma, dma((pieces,)), dma((pieces,)),
            dma((peers - 1,)), dma((peers - 1,)),
        ],
        compiler_params=pltpu.CompilerParams(
            collective_id=0, has_side_effects=True, vmem_limit_bytes=67043328
        ),
        name="layer",
    )(
        head_inputs, gate_inputs, step_raw.T, decay_log.reshape(1, -1),
        state_write, state_read, skip_gain.reshape(1, -1), norm_gain.reshape(1, -1),
    )
    part = 2
    wide = pl.BlockSpec((part * L, inner), lambda c: (c, 0))
    return pl.pallas_call(
        functools.partial(scale_kernel, part, norm_gain.shape[0]),
        grid=(chunks // part,),
        in_specs=[wide, pl.BlockSpec((chunks, L), lambda c: (0, 0))],
        out_specs=wide,
        out_shape=sds((tokens, inner), BF16),
        name="scale",
    )(gated, squares)


def solution(mesh):
    return jax.shard_map(
        functools.partial(on_device, mesh.shape["seq"], mesh.shape["head"]),
        mesh=mesh,
        in_specs=(
            P("seq", "head"),
            P("seq", "head"),
            P("seq", "head"),
            P(),
            P(("seq", "head"), None),
            P(("seq", "head"), None),
            P(),
            P(),
        ),
        out_specs=P("seq", "head"),
        check_vma=False,
    )
```

```python
import functools
import math

import jax
import jax.numpy as jnp
from jax import lax
from jax.experimental import pallas as pl
from jax.experimental.pallas import tpu as pltpu
from jax.sharding import PartitionSpec as P

HEAD_DIM = 64
L = 128
SLOT = 32
LOG2E = math.log2(math.e)
F32 = jnp.float32
BF16 = jnp.bfloat16
MESH = pl.DeviceIdType.MESH
CAP = 100.0
UNROLL = 4
LEAD = 3
HOP = 3


def pair_lanes(first, second, rows):
    lane = lax.broadcasted_iota(jnp.int32, (rows, L), 1)
    first = jnp.broadcast_to(first, (rows, L))
    second = jnp.broadcast_to(second, (rows, L))
    return jnp.where(lane < HEAD_DIM, first, second)


def layer_kernel(
    count, peers, heads, tiles, group, chunks,
    x_hbm, z_hbm, raw_hbm, decay_hbm, write_hbm, read_hbm, skip_hbm, gain_hbm,
    gated_hbm, square_ref, gated_ref, out_sem, raw_ref, decay_ref, skip_ref, gain_ref, writes_t,
    x_ref, z_ref, writes, reads, sums, run_rows, cols, masked, local,
    loc, pre, fin, carry, tot, mate_buf, mate_tot, chain_in, chain_out, coming_ref,
    spot, sq, sq_own, sq_in,
    x_sem, z_sem, in_sem, s_w, r_w, s_r, r_r, s_mate, r_mate, s_tot, r_tot, s_chain, r_chain, s_sq, r_sq,
):
    me = lax.axis_index("seq")
    head = lax.axis_index("head")
    odd = lax.rem(me, 2)
    is_odd = odd == 1
    pairs = count // 2
    place = me // 2
    mate = me + 1 - 2 * odd
    after = lax.rem(me + 2, count)
    before = lax.rem(me + count - 2, count)
    has_before = place > 0
    has_after = place < pairs - 1
    pieces = tiles // group
    width = group * L
    rows = write_hbm.shape[0]
    own_rows = pl.ds(pl.multiple_of(head * rows, L), rows)
    inputs = [
        pltpu.make_async_copy(source, target, in_sem.at[i])
        for i, (source, target) in enumerate(
            [
                (write_hbm, writes.at[own_rows]),
                (read_hbm, reads.at[own_rows]),
                (raw_hbm, raw_ref),
                (decay_hbm, decay_ref),
                (skip_hbm, skip_ref),
                (gain_hbm, gain_ref),
            ]
        )
    ]
    for copy in inputs:
        copy.start()

    def load_x(p):
        span = pl.ds(p * width, width)
        return pltpu.make_async_copy(x_hbm.at[:, span], x_ref.at[:, span], x_sem.at[p])

    def store(p):
        span = pl.ds(p * width, width)
        return pltpu.make_async_copy(
            gated_ref.at[:, span], gated_hbm.at[:, span], out_sem.at[p]
        )

    load_z = pltpu.make_async_copy(z_hbm, z_ref, z_sem)
    for p in range(pieces):
        load_x(p).start()
    load_z.start()

    barrier = pltpu.get_barrier_semaphore()
    for other in (mate, after, before):
        pl.semaphore_signal(barrier, inc=1, device_id={"seq": other}, device_id_type=MESH)
    for d in range(1, peers):
        pl.semaphore_signal(
            barrier, inc=1, device_id={"head": lax.rem(head + d, peers)}, device_id_type=MESH
        )
    pl.semaphore_wait(barrier, 3 + peers - 1)

    def to_peer(src, dst, send, recv, d):
        return pltpu.make_async_remote_copy(
            src_ref=src, dst_ref=dst, send_sem=send.at[d - 1], recv_sem=recv.at[d - 1],
            device_id={"head": lax.rem(head + d, peers)}, device_id_type=MESH,
        )

    give_w = [to_peer(writes.at[own_rows], writes.at[own_rows], s_w, r_w, d) for d in range(1, peers)]
    give_r = [to_peer(reads.at[own_rows], reads.at[own_rows], s_r, r_r, d) for d in range(1, peers)]
    inputs[0].wait()
    for copy in give_w:
        copy.start()
    inputs[1].wait()
    for copy in give_r:
        copy.start()
    for copy in inputs[2:]:
        copy.wait()

    total_heads = decay_ref.shape[1]
    spot[...] = jnp.zeros_like(spot)
    spot[0:1, :total_heads] = decay_ref[...]
    spot[1:2, :total_heads] = skip_ref[...]
    rolled = pltpu.roll(spot[...], lax.rem(L - head * heads, L), 1)
    skip_row = rolled[1:2, :]
    square = jnp.broadcast_to(rolled[0:1, :], (L, L)).T
    rate = jnp.exp(square[:heads, :1]) * LOG2E
    raw = raw_ref[...].astype(F32)
    step = jnp.maximum(raw, 0.0) + jnp.log1p(jnp.exp(-jnp.abs(raw)))
    falls = -rate * step
    steps = jnp.log2(step)
    sums[...] = jnp.zeros_like(sums)
    for c in range(chunks):
        sums[c, :heads, :] = falls[:, c * L : (c + 1) * L]
    row = lax.broadcasted_iota(jnp.int32, (L, L), 0)
    col = lax.broadcasted_iota(jnp.int32, (L, L), 1)
    upper = jnp.where(row <= col, 1.0, 0.0).astype(F32)
    run_all = jnp.dot(
        sums[...].reshape(chunks * SLOT, L), upper,
        preferred_element_type=F32, precision=lax.Precision.HIGHEST,
    ).reshape(chunks, SLOT, L)
    sums[:, :, :] = jnp.zeros_like(sums)
    for c in range(chunks):
        sums[c, :heads, :] = steps[:, c * L : (c + 1) * L]
    tot[...] = jnp.zeros_like(tot)
    for c in range(chunks):
        run = run_all[c]
        run_u = run - sums[c]
        run_rows[c] = run_u
        last = jnp.broadcast_to(run[:, L - 1 : L], (SLOT, L))
        cols[c] = jnp.concatenate(
            [run, jnp.exp2(run), jnp.exp2(last - run_u), last], axis=0
        ).T
        pre[c] = tot[...]
        for j in range(tiles):
            at = 3 * SLOT + 2 * j
            gone = pair_lanes(cols[c, 0:1, at : at + 1], cols[c, 0:1, at + 1 : at + 2], 1)
            tot[j : j + 1, :] = tot[j : j + 1, :] + gone

    tot_copy = pltpu.make_async_remote_copy(
        src_ref=tot, dst_ref=mate_tot, send_sem=s_tot, recv_sem=r_tot,
        device_id={"seq": mate}, device_id_type=MESH,
    )
    tot_copy.start()
    for copy in give_w:
        copy.wait_recv()
    for c in range(chunks):
        writes_t[c] = writes[c * L : (c + 1) * L, :].astype(F32).T.astype(BF16)

    def to_mate(p):
        part = pl.ds(p * group, group)
        return pltpu.make_async_remote_copy(
            src_ref=fin.at[part], dst_ref=mate_buf.at[part],
            send_sem=s_mate.at[p], recv_sem=r_mate.at[p],
            device_id={"seq": mate}, device_id_type=MESH,
        )

    def to_next(p):
        part = pl.ds(p * group, group)
        return pltpu.make_async_remote_copy(
            src_ref=chain_out.at[part], dst_ref=chain_in.at[part],
            send_sem=s_chain.at[p], recv_sem=r_chain.at[p],
            device_id={"seq": after}, device_id_type=MESH,
        )

    def at_chunk(c):
        return pl.ds(pl.multiple_of(c * L, L), L)

    def chain_step(p):
        to_mate(p).wait_recv()

        @pl.when(has_before)
        def _():
            to_next(p).wait_recv()

        for i in range(group):
            j = p * group + i
            own_tot = jnp.exp2(tot[pl.ds(j, 1), :])
            other_tot = jnp.exp2(mate_tot[pl.ds(j, 1), :])
            own = fin[j].astype(F32)
            other = mate_buf[j].astype(F32)
            coming = chain_in[j].astype(F32)
            early = jnp.where(is_odd, other, own)
            late = jnp.where(is_odd, own, other)
            early_tot = jnp.where(is_odd, other_tot, own_tot)
            late_tot = jnp.where(is_odd, own_tot, other_tot)
            middle = early_tot * coming + early
            chain_out[j] = (late_tot * middle + late).astype(BF16)
            coming_ref[j] = jnp.where(is_odd, middle, coming)

        @pl.when(has_after)
        def _():
            to_next(p).start()

    def maybe_step(slot):
        due = slot - shift

        @pl.when(jnp.logical_and(due >= 0, due < pieces))
        def _():
            chain_step(due)

    lead = min(LEAD, pieces)
    shift = jnp.minimum(lead + HOP * place, 2 * pieces)

    @pl.when(jnp.logical_not(has_before))
    def _():
        chain_in[...] = jnp.zeros_like(chain_in)

    for p in range(pieces):
        if p == lead:
            tot_copy.wait_recv()
        if p >= lead:
            maybe_step(p)
        load_x(p).wait()
        carry[...] = jnp.zeros_like(carry)

        def advance(c, _, p=p):
            here = at_chunk(c)
            tail = cols[c]
            weighted = []
            for j in range(p * group, (p + 1) * group):
                at = 2 * SLOT + 2 * j
                wide = pair_lanes(tail[:, at : at + 1], tail[:, at + 1 : at + 2], L)
                x = x_ref[here, j * L : (j + 1) * L].astype(F32)
                weighted.append((wide * x).astype(BF16))
            new = jnp.dot(
                writes_t[c], jnp.concatenate(weighted, axis=1), preferred_element_type=F32
            )
            for i in range(group):
                j = p * group + i
                at = 3 * SLOT + 2 * j
                gone = pair_lanes(tail[0:1, at : at + 1], tail[0:1, at + 1 : at + 2], 1)
                old = carry[i]
                loc[c, j] = old.astype(BF16)
                carry[i] = jnp.exp2(gone) * old + new[:, i * L : (i + 1) * L]
            return 0

        lax.fori_loop(0, chunks, advance, 0, unroll=UNROLL)
        for i in range(group):
            fin[p * group + i] = carry[i].astype(BF16)
        to_mate(p).start()

    if lead >= pieces:
        tot_copy.wait_recv()
    for copy in give_r:
        copy.wait_recv()

    def score(c, _):
        here = at_chunk(c)
        scores = lax.dot_general(
            reads[here, :], writes[here, :], (((1,), (1,)), ((), ())),
            preferred_element_type=F32,
        )
        masked[c] = jnp.where(col <= row, scores, 0.0)
        return 0

    lax.fori_loop(0, chunks, score, 0, unroll=UNROLL)
    left = col < HEAD_DIM
    for k in range(pieces):
        maybe_step(pieces + k)

        def inside(c, _, p=k):
            here = at_chunk(c)
            run = cols[c]
            scores = masked[c]
            for j in range(p * group, (p + 1) * group):
                x = x_ref[here, j * L : (j + 1) * L].astype(F32)
                mixes = []
                for h in (2 * j, 2 * j + 1):
                    spread = run[:, h : h + 1] - run_rows[c, h : h + 1, :]
                    mixes.append((scores * jnp.exp2(jnp.minimum(spread, CAP))).astype(BF16))
                top = jnp.where(left, x, 0.0).astype(BF16)
                bottom = jnp.where(left, 0.0, x).astype(BF16)
                skip = pair_lanes(
                    skip_row[:, 2 * j : 2 * j + 1], skip_row[:, 2 * j + 1 : 2 * j + 2], 1
                )
                local[here, j * L : (j + 1) * L] = skip * x + jnp.dot(
                    jnp.concatenate(mixes, axis=1), jnp.concatenate([top, bottom], axis=0),
                    preferred_element_type=F32,
                )
            return 0

        lax.fori_loop(0, chunks, inside, 0, unroll=UNROLL)

    load_z.wait()
    sq[...] = jnp.zeros_like(sq)
    first_gain = pl.multiple_of(head * (tiles * L), L)
    for k in range(pieces):

        @pl.when(k + shift >= 2 * pieces)
        def _():
            chain_step(jnp.int32(k))

        gain = gain_ref[:, pl.ds(first_gain + k * width, width)]

        def finish(c, _, p=k, gain=gain):
            here = at_chunk(c)
            grown = cols[c]
            entering = []
            for j in range(p * group, (p + 1) * group):
                entering.append(
                    (
                        loc[c, j].astype(F32) + jnp.exp2(pre[c, j : j + 1, :]) * coming_ref[j]
                    ).astype(BF16)
                )
            inter = jnp.dot(
                reads[here, :], jnp.concatenate(entering, axis=1), preferred_element_type=F32
            )
            squares = sq[c]
            for i in range(group):
                j = p * group + i
                at = SLOT + 2 * j
                span = slice(j * L, (j + 1) * L)
                y = local[here, span] + (
                    pair_lanes(grown[:, at : at + 1], grown[:, at + 1 : at + 2], L)
                    * inter[:, i * L : (i + 1) * L]
                )
                z = z_ref[here, span].astype(F32)
                gated = y * z * jax.nn.sigmoid(z)
                squares = squares + gated * gated
                gated_ref[here, span] = (gated * gain[:, i * L : (i + 1) * L]).astype(BF16)
            sq[c] = squares
            return 0

        lax.fori_loop(0, chunks, finish, 0, unroll=UNROLL)
        store(k).start()

    for c in range(chunks):
        sq_own[c : c + 1, :] = jnp.sum(sq[c].T, axis=0, keepdims=True)
    give_sq = [to_peer(sq_own, sq_in.at[d - 1], s_sq, r_sq, d) for d in range(1, peers)]
    for copy in give_sq:
        copy.start()
    square_sum = sq_own[...]
    for d in range(1, peers):
        give_sq[d - 1].wait_recv()
        square_sum = square_sum + sq_in[d - 1]
    square_ref[...] = square_sum

    tot_copy.wait_send()
    for copy in give_w + give_r + give_sq:
        copy.wait_send()
    for p in range(pieces):
        store(p).wait()
        to_mate(p).wait_send()

        @pl.when(has_after)
        def _():
            to_next(p).wait_send()


def scale_kernel(part, channels, gated_ref, square_ref, out_ref):
    i = pl.program_id(0)
    for k in range(part):
        sums = square_ref[pl.ds(i * part + k, 1), :]
        factor = lax.rsqrt(jnp.broadcast_to(sums, (L, L)).T / channels + 1e-05)
        here = slice(k * L, (k + 1) * L)
        for j in range(gated_ref.shape[1] // L):
            span = slice(j * L, (j + 1) * L)
            out_ref[here, span] = (gated_ref[here, span].astype(F32) * factor).astype(BF16)


def on_device(
    count, peers, head_inputs, gate_inputs, step_raw, decay_log, state_write, state_read, skip_gain, norm_gain
):
    tokens, inner = head_inputs.shape
    heads = inner // HEAD_DIM
    tiles = inner // L
    chunks = tokens // L
    states = state_write.shape[1]
    group = math.gcd(tiles, 2)
    pieces = tiles // group
    sds = jax.ShapeDtypeStruct
    vmem = pl.BlockSpec(memory_space=pltpu.VMEM)
    hbm = pl.BlockSpec(memory_space=pltpu.HBM)
    dma = pltpu.SemaphoreType.DMA
    state = (tiles, states, L)
    gated, squares = pl.pallas_call(
        functools.partial(layer_kernel, count, peers, heads, tiles, group, chunks),
        in_specs=[hbm] * 8,
        out_specs=[hbm, vmem],
        out_shape=[sds((tokens, inner), BF16), sds((chunks, L), F32)],
        scratch_shapes=[
            pltpu.VMEM((tokens, inner), BF16),
            dma((pieces,)),
            pltpu.VMEM((heads, tokens), BF16),
            pltpu.VMEM((1, decay_log.shape[0]), F32),
            pltpu.VMEM((1, skip_gain.shape[0]), F32),
            pltpu.VMEM((1, norm_gain.shape[0]), F32),
            pltpu.VMEM((chunks, states, L), BF16),
            pltpu.VMEM((tokens, inner), BF16),
            pltpu.VMEM((tokens, inner), BF16),
            pltpu.VMEM((tokens, states), BF16),
            pltpu.VMEM((tokens, states), BF16),
            pltpu.VMEM((chunks, SLOT, L), F32),
            pltpu.VMEM((chunks, SLOT, L), F32),
            pltpu.VMEM((chunks, L, L), F32),
            pltpu.VMEM((chunks, L, L), F32),
            pltpu.VMEM((tokens, inner), F32),
            pltpu.VMEM((chunks,) + state, BF16),
            pltpu.VMEM((chunks, tiles, L), F32),
            pltpu.VMEM(state, BF16),
            pltpu.VMEM((group, states, L), F32),
            pltpu.VMEM((tiles, L), F32),
            pltpu.VMEM(state, BF16),
            pltpu.VMEM((tiles, L), F32),
            pltpu.VMEM(state, BF16),
            pltpu.VMEM(state, BF16),
            pltpu.VMEM(state, F32),
            pltpu.VMEM((8, L), F32),
            pltpu.VMEM((chunks, L, L), F32),
            pltpu.VMEM((chunks, L), F32),
            pltpu.VMEM((peers - 1, chunks, L), F32),
            dma((pieces,)), dma, dma((6,)),
            dma((peers - 1,)), dma((peers - 1,)), dma((peers - 1,)), dma((peers - 1,)),
            dma((pieces,)), dma((pieces,)), dma, dma, dma((pieces,)), dma((pieces,)),
            dma((peers - 1,)), dma((peers - 1,)),
        ],
        compiler_params=pltpu.CompilerParams(
            collective_id=0, has_side_effects=True, vmem_limit_bytes=67043328
        ),
        name="layer",
    )(
        head_inputs, gate_inputs, step_raw.T, decay_log.reshape(1, -1),
        state_write, state_read, skip_gain.reshape(1, -1), norm_gain.reshape(1, -1),
    )
    part = 2
    wide = pl.BlockSpec((part * L, inner), lambda c: (c, 0))
    return pl.pallas_call(
        functools.partial(scale_kernel, part, norm_gain.shape[0]),
        grid=(chunks // part,),
        in_specs=[wide, pl.BlockSpec((chunks, L), lambda c: (0, 0))],
        out_specs=wide,
        out_shape=sds((tokens, inner), BF16),
        name="scale",
    )(gated, squares)


def solution(mesh):
    return jax.shard_map(
        functools.partial(on_device, mesh.shape["seq"], mesh.shape["head"]),
        mesh=mesh,
        in_specs=(
            P("seq", "head"),
            P("seq", "head"),
            P("seq", "head"),
            P(),
            P(("seq", "head"), None),
            P(("seq", "head"), None),
            P(),
            P(),
        ),
        out_specs=P("seq", "head"),
        check_vma=False,
    )
```
